32 devices in a mesh: band: 8 (over z, x), grid: 4 (over y, core).
Axes of the slice: x: 2, y: 2, z: 4, core: 2. Of those that a mesh axis runs over, the one named last changes fastest.
Arguments:
- partial_density: float32 [8, 128, 128, 128], P('band', 'grid'), may hold values from 0.01 to 1
- node_index: int32 [128, 128, 128], P('grid'), may hold values from 0 to 19
- node_weight: float32 [4, 128, 128, 128], P(None, 'grid'), may hold values from 0 to 1
- node_slope: float32 [4, 128, 128, 128], P(None, 'grid'), may hold values from -6 to 6
- kernel_table: float32 [20, 20, 114], replicated, may hold values from -0.8 to 0.8, as said below
Outputs:
- potential: float32 [128, 128, 128], P('grid')
The draws below stay inside these ranges and needn't reach their ends.
Inputs may be any that keep to these rules, and one draw needn't show every extreme that they name: node_index(r) is the node at the lower end of the interval of q0 at r; nodes node_index - 1 to node_index + 2 carry the four weights. `kernel_table`: symmetric in its first two indices.
All inputs are finite; a program needn't handle non-finite values.
Results may differ from the reference program's by a relative error of at most 0.0003.
Values sent between devices are 32-bit elements; how exact they have to be, the bound alone decides.
A program may use at most 128 MiB of HBM per device.

```python
import math
import jax
import jax.numpy as jnp
from jax import lax

N = 128
NA = 20
SHELLS = 114
GROUPS = 8


def draw_kernel_table(key, part):
    sample_values = jax.random.truncated_normal(key, -4.0, 4.0, (NA, NA, SHELLS), jnp.float32) * 0.2
    symmetric = 0.5 * (sample_values + jnp.transpose(sample_values, (1, 0, 2)))
    return symmetric


def touch_ends(array, own_key, least, largest):
    place = [jax.random.randint(jax.random.fold_in(own_key, axis), (), 0, length) for axis, length in enumerate(array.shape)]
    widest = array.shape.index(max(array.shape))
    next_to = place[:widest] + [(place[widest] + 1) % array.shape[widest]] + place[widest + 1:]
    return array.at[tuple(place)].set(least).at[tuple(next_to)].set(largest)


def block_scale(own_key, extent, split, smallest, high):
    level = 1.0
    for position, parts in split:
        steps = jax.random.uniform(jax.random.fold_in(jax.random.fold_in(own_key, 6), position), (parts,), jnp.float32, smallest / len(split), high / len(split))
        level = level * jnp.repeat(jnp.exp(steps), extent[position] // parts).reshape((-1,) + (1,) * (len(extent) - 1 - position))
    return level


def noise(key, shape, width, reach, pieces=(), kind=jnp.bfloat16):
    drawn = width * jax.random.normal(key, shape, jnp.float32)
    if pieces:
        drawn = drawn * block_scale(key, shape, pieces, -0.22, 0.18)
    return jnp.clip(drawn, -reach, reach).astype(kind)


def setup_inputs(seed: int = 0) -> dict:
    seeds = jax.random.split(jax.random.key(seed), 6)
    partial_density = jnp.clip(jnp.exp(math.log(1.0) - 4.6051702 * jax.random.uniform(seeds[0], (GROUPS, N, N, N), jnp.float32) ** block_scale(seeds[0], (GROUPS, N, N, N), ((0, 8), (1, 4)), -0.2, 0.2)), 0.01, 1.0)
    node_index = touch_ends(jax.random.randint(seeds[1], (N, N, N), 0, NA), jax.random.fold_in(seeds[1], 1), 0, NA - 1).astype(jnp.int32)
    node_weight = jnp.clip(1.0 * jax.random.uniform(seeds[2], (4, N, N, N), jnp.float32) ** block_scale(seeds[2], (4, N, N, N), ((1, 4),), -0.2, 0.2), 0.0, 1.0)
    node_slope = noise(seeds[3], (4, N, N, N), 1.0, 6.0, ((1, 4),), jnp.float32)
    kernel_table = draw_kernel_table(jax.random.fold_in(seeds[5], 71), 0)
    return {"partial_density": partial_density, "node_index": node_index, "node_weight": node_weight, "node_slope": node_slope, "kernel_table": kernel_table}


def frequency(length):
    positions = jnp.arange(length, dtype=jnp.int32)
    return jnp.where(positions < length // 2, positions, positions - length)

def shell_split(square_norm):
    root_value = jnp.sqrt(square_norm.astype(jnp.float32))
    shell_idx = root_value.astype(jnp.int32)
    shell_idx = shell_idx - (shell_idx * shell_idx > square_norm).astype(jnp.int32)
    shell_idx = shell_idx + ((shell_idx + 1) * (shell_idx + 1) <= square_norm).astype(jnp.int32)
    fraction = root_value - shell_idx.astype(jnp.float32)
    return (shell_idx, fraction)

def node_fields(count_nodes, intervals, weights):
    node_ids = jnp.arange(count_nodes, dtype=jnp.int32)
    summed = jnp.zeros((count_nodes,) + intervals.shape, jnp.float32)
    for offset in range(4):
        matched = node_ids[:, None, None, None] == (intervals + (offset - 1))[None]
        summed = summed + jnp.where(matched, weights[offset][None], jnp.zeros((), jnp.float32))
    return summed

def reference(partial_density, node_index, node_weight, node_slope, kernel_table):
    density = lax.optimization_barrier(jnp.sum(partial_density, axis=0))
    theta_fields = density[None] * node_fields(NA, node_index, node_weight)
    spectrum = jnp.fft.fftn(theta_fields, axes=(1, 2, 3))
    spec_real = jnp.real(spectrum)
    spec_imag = jnp.imag(spectrum)
    freq_all = frequency(N)
    plane_norm = freq_all[:, None] * freq_all[:, None] + freq_all[None, :] * freq_all[None, :]

    def mix_plane(plane_idx):
        freq_x = freq_all[plane_idx]
        shell_idx, fraction = shell_split(plane_norm + freq_x * freq_x)
        lower_values = kernel_table[:, :, shell_idx]
        upper_values = kernel_table[:, :, shell_idx + 1]
        kernel = (1.0 - fraction) * lower_values + fraction * upper_values
        plane_real = lax.dynamic_index_in_dim(spec_real, plane_idx, 1, keepdims=False)
        plane_imag = lax.dynamic_index_in_dim(spec_imag, plane_idx, 1, keepdims=False)
        out_real = jnp.einsum('abyz,ayz->byz', kernel, plane_real, precision=lax.Precision.HIGHEST)
        out_imag = jnp.einsum('abyz,ayz->byz', kernel, plane_imag, precision=lax.Precision.HIGHEST)
        return (out_real, out_imag)
    mixed_real, mixed_imag = lax.map(mix_plane, jnp.arange(N, dtype=jnp.int32))
    mixed = jnp.moveaxis(mixed_real + 1j * mixed_imag, 0, 1)
    fields = jnp.real(jnp.fft.ifftn(mixed, axes=(1, 2, 3)))
    return lax.optimization_barrier(jnp.sum(fields * node_fields(NA, node_index, node_slope), axis=0))
```

```python
import math

import jax
import jax.numpy as jnp
from jax import lax
from jax.experimental import pallas as pl
from jax.experimental.pallas import tpu as pltpu
from jax.sharding import PartitionSpec as P

def frequency_of(positions, length):
    return jnp.where(positions < length // 2, positions, positions - length)


def shell_split(square_norm):
    root_value = jnp.sqrt(square_norm.astype(jnp.float32))
    shell_idx = root_value.astype(jnp.int32)
    shell_idx = shell_idx - (shell_idx * shell_idx > square_norm).astype(jnp.int32)
    shell_idx = shell_idx + ((shell_idx + 1) * (shell_idx + 1) <= square_norm).astype(jnp.int32)
    fraction = root_value - shell_idx.astype(jnp.float32)
    return (shell_idx, fraction)


def node_fields(count_nodes, intervals, weights):
    node_ids = jnp.arange(count_nodes, dtype=jnp.int32)
    summed = jnp.zeros((count_nodes,) + intervals.shape, jnp.float32)
    for offset in range(4):
        matched = node_ids[:, None, None, None] == (intervals + (offset - 1))[None]
        summed = summed + jnp.where(matched, weights[offset][None], jnp.zeros((), jnp.float32))
    return summed


def phase_table(source_idx, target_idx, modulus):
    product_mod = source_idx[:, None] * target_idx[None, :] % modulus
    angles = product_mod.astype(jnp.float32) * (2.0 * math.pi / modulus)
    return (jnp.cos(angles), jnp.sin(angles))


def contract(pattern, operand, matrix):
    return jnp.einsum(pattern, operand, matrix, precision=lax.Precision.HIGHEST)


def mirrored(values, dim):
    return jnp.roll(jnp.flip(values, dim), 1, dim)


def forward_tables(positions, plane_ids, length):
    cosine, sine = phase_table(positions, plane_ids, length)
    alternating = jnp.where(positions % 2 == 0, 1.0, -1.0).astype(jnp.float32)
    sine = jnp.where(plane_ids[None, :] == 0, -alternating[:, None], sine)
    return (cosine, sine)


def shell_weights_of(square_norm, shell_count):
    shell_ids = jnp.arange(shell_count, dtype=jnp.int32)
    shell_idx, fraction = shell_split(square_norm)
    expand = (slice(None),) + (None,) * square_norm.ndim
    lower_hit = shell_ids[expand] == shell_idx[None]
    upper_hit = shell_ids[expand] == shell_idx[None] + 1
    return jnp.where(lower_hit, 1.0 - fraction[None], 0.0) + jnp.where(
        upper_hit, fraction[None], 0.0
    )


def short(pattern, left, right):
    return jnp.einsum(pattern, left, right, precision=lax.Precision.HIGH)


def halves(values):
    high = values.astype(jnp.bfloat16)
    low = (values - high.astype(jnp.float32)).astype(jnp.bfloat16)
    return high, low


def mix_kernel(count, padded, shell_ref, frac_ref, table_ref, spec_ref, out_ref):
    rows, lanes = shell_ref.shape[1:]
    ids = lax.broadcasted_iota(jnp.int32, (table_ref.shape[1] // 3, lanes), 0)

    def hats(row):
        shell = shell_ref[0, pl.ds(row, 1), :]
        frac = frac_ref[0, pl.ds(row, 1), :]
        return jnp.where(ids == shell, 1.0 - frac, jnp.where(ids == shell + 1, frac, 0.0))

    def step(pair, carry):
        both = jnp.concatenate([hats(2 * pair), hats(2 * pair + 1)], axis=1)
        high, low = halves(both)
        phi = jnp.dot(
            table_ref[...],
            jnp.concatenate([high, high, low], axis=0),
            preferred_element_type=jnp.float32,
        )
        for side in range(2):
            row = 2 * pair + side
            real = jnp.zeros((padded, lanes), jnp.float32)
            imag = jnp.zeros((padded, lanes), jnp.float32)
            for node in range(count):
                part = phi[node * padded : (node + 1) * padded, side * lanes : (side + 1) * lanes]
                real = real + part * spec_ref[0, node, 0, pl.ds(row, 1), :]
                imag = imag + part * spec_ref[1, node, 0, pl.ds(row, 1), :]
            out_ref[0, row, 0] = real[:count]
            out_ref[0, row, 1] = imag[:count]
        return carry

    lax.fori_loop(0, rows // 2, step, 0)


def mix(spectrum, shell, frac, kernel_table):
    _, count, planes, rows, lanes = spectrum.shape
    padded = -(-count // 8) * 8
    depth = -(-(kernel_table.shape[2]) // 128) * 128
    table = jnp.pad(kernel_table, ((0, 0), (0, padded - count), (0, depth - kernel_table.shape[2])))
    table = table.reshape(count * padded, depth)
    rounded = lax.reduce_precision(table, exponent_bits=8, mantissa_bits=7)
    high, low = rounded.astype(jnp.bfloat16), (table - rounded).astype(jnp.bfloat16)
    table = jnp.concatenate([high, low, high], axis=1)
    return pl.pallas_call(
        lambda *refs: mix_kernel(count, padded, *refs),
        grid=(planes,),
        in_specs=[
            pl.BlockSpec((1, rows, lanes), lambda p: (p, 0, 0)),
            pl.BlockSpec((1, rows, lanes), lambda p: (p, 0, 0)),
            pl.BlockSpec(table.shape, lambda p: (0, 0)),
            pl.BlockSpec((2, count, 1, rows, lanes), lambda p: (0, 0, p, 0, 0)),
        ],
        out_specs=pl.BlockSpec((1, rows, 2, count, lanes), lambda p: (p, 0, 0, 0, 0)),
        out_shape=jax.ShapeDtypeStruct((planes, rows, 2, count, lanes), jnp.float32),
    )(shell, frac, table, spectrum)


def per_device(partial_density, node_index, node_weight, node_slope, kernel_table):
    length = node_index.shape[1]
    half = length // 2
    count_nodes = kernel_table.shape[0]
    shell_count = kernel_table.shape[2]
    planes = half // lax.axis_size("band")
    grid_size = lax.axis_size("grid")
    grid_part = length // grid_size
    band_at = lax.axis_index("band")
    grid_at = lax.axis_index("grid")
    full_range = jnp.arange(length, dtype=jnp.int32)
    own_planes = band_at * planes + jnp.arange(planes, dtype=jnp.int32)
    own_rows = grid_at * grid_part + jnp.arange(grid_part, dtype=jnp.int32)
    lower = ((full_range >= 1) & (full_range < half)).astype(jnp.float32)
    upper = (full_range > half).astype(jnp.float32)
    single = 1.0 - lower - upper
    joint = (own_planes == 0)[:, None, None, None, None]
    cosine, sine = phase_table(full_range, full_range, length)
    forward = jnp.stack(
        [jnp.stack([cosine, -sine], 1), jnp.stack([sine, cosine], 1)]
    )
    low_only = lower + single
    packed = jnp.stack(
        [
            jnp.stack([cosine * low_only, -sine * lower], 1),
            jnp.stack([cosine * upper, -sine * upper + cosine * single], 1),
        ]
    )
    forward_y = jnp.where(joint, packed[None], forward[None])
    backward = jnp.stack(
        [jnp.stack([cosine, sine], 1), jnp.stack([-sine, cosine], 1)]
    )
    lower_col, upper_col, single_col = (v[:, None] for v in (lower, upper, single))
    opened = jnp.stack(
        [
            jnp.stack([cosine * (2.0 * lower_col + single_col), cosine * (2.0 * upper_col)], 1),
            jnp.stack(
                [sine * (-2.0 * lower_col), sine * (-2.0 * upper_col) + cosine * single_col], 1
            ),
        ]
    )
    backward_y = jnp.where(joint, opened[None], backward[None])

    density = lax.psum(partial_density[0], "band")
    theta_fields = density[None] * node_fields(count_nodes, node_index, node_weight)
    cosine_z, sine_z = forward_tables(full_range, own_planes, length)
    table_z = jnp.stack([cosine_z, -sine_z], 1)
    columns = short("zcp,axyz->cpaxy", table_z, theta_fields)
    waves = short("cpaxy,pcydw->wdapx", columns, forward_y)
    waves = waves.reshape((grid_size, grid_part) + waves.shape[1:])
    pencils = lax.all_to_all(waves, "grid", split_axis=0, concat_axis=0, tiled=True)
    forward_x = forward.reshape((2, grid_size, grid_part) + forward.shape[2:])
    spectrum = short("gwdapx,dgxev->eapwv", pencils, forward_x)

    freq_x = frequency_of(full_range, length)
    square_x = freq_x * freq_x
    freq_rows = frequency_of(own_rows, length)
    square_rows = freq_rows * freq_rows
    third_square = jnp.where(
        (own_planes[:, None] == 0) & (own_rows[None, :] > half),
        half * half,
        (own_planes * own_planes)[:, None],
    )
    square_norm = (third_square + square_rows[None, :])[:, :, None] + square_x
    shell, frac = shell_split(square_norm)
    mixed = mix(spectrum, shell, frac, kernel_table)

    flag = ((own_rows[0] == 0) | (own_rows[0] == half)) & (own_planes[0] == 0)
    first_norm = square_x + square_rows[0]
    pair_norm = jnp.stack([first_norm, first_norm + half * half])
    kernels = contract("abs,sqx->qabx", kernel_table, shell_weights_of(pair_norm, shell_count))
    spread = (0.5 * flag.astype(jnp.float32)) * (kernels[0] - kernels[1])
    base = spectrum[:, :, 0, 0, :]
    turned = mirrored(base, 2)
    delta = jnp.stack([turned[0] - base[0], -turned[1] - base[1]])
    extra = jnp.sum(spread[None] * delta[:, :, None, :], axis=1)
    mixed = mixed.at[0, 0].add(extra)

    backward_x = backward.reshape(2, length, 2, grid_size, grid_part)
    inverse = short("pwdbv,dvegx->gwebpx", mixed, backward_x)
    returned = lax.all_to_all(inverse, "grid", split_axis=0, concat_axis=0, tiled=True)
    backward_y = backward_y.reshape((planes, 2, grid_size, grid_part, 2, length))
    slab = short("gwdbpx,pdgwcy->cpbxy", returned, backward_y)
    cosine_own, sine_own = phase_table(own_planes, full_range, length)
    alternating = jnp.where(full_range % 2 == 0, 1.0, -1.0).astype(jnp.float32)
    cosine_back = jnp.where(own_planes[:, None] == 0, 1.0, 2.0 * cosine_own)
    sine_back = jnp.where(own_planes[:, None] == 0, -alternating[None, :], 2.0 * sine_own)
    table_back = jnp.stack([cosine_back, -sine_back]) * (1.0 / float(length) ** 3)
    field_parts = short("cpbxy,cpz->bxyz", slab, table_back)
    slopes = node_fields(count_nodes, node_index, node_slope)
    partial_potential = jnp.sum(field_parts * slopes, axis=0)
    return lax.psum(partial_potential, "band")


def solution(mesh):
    placed = (
        P("band", "grid", None, None),
        P("grid", None, None),
        P(None, "grid", None, None),
        P(None, "grid", None, None),
        P(),
    )
    return jax.shard_map(
        per_device, mesh=mesh, in_specs=placed, out_specs=P("grid", None, None), check_vma=False
    )
```
